128 devices in a mesh: row: 16 (over z, y), col: 8 (over x, core).
Axes of the slice: x: 4, y: 4, z: 4, core: 2. Of those that a mesh axis runs over, the one named last changes fastest.
Arguments:
- pair: bfloat16 [768, 768, 128], P('row', 'col'), may hold values from -6 to 6
- chain_lengths: int32 [8], replicated, may hold values from 1 to 96, 576 in all
- gains: float32 [2, 2, 128], replicated, may hold values from 0.1 to 1.9
- biases: float32 [2, 2, 128], replicated, may hold values from -3 to 3
- w_in: bfloat16 [2, 128, 640], replicated, may hold values from -0.5 to 0.5
- w_out: bfloat16 [2, 128, 128], replicated, may hold values from -0.5 to 0.5
Outputs:
- pair_out: bfloat16 [768, 768, 128], P('row', 'col')
The draws below stay inside these ranges and needn't reach their ends.
Inputs may be any that keep to these rules, and one draw needn't show every extreme that they name: Chain k occupies positions k * 96 to (k + 1) * 96 - 1 and its live residues are the first chain_lengths[k] of them; the lengths sum to 576 and one of them equals 96.
All inputs are finite; a program needn't handle non-finite values.
Results may differ from the reference program's by a relative error of at most 0.0054.
Values may be sent and summed in bfloat16 or wider, within the bound.
No kernel may reach another device: no remote copies, remote signals or barrier semaphores. Data moves between devices by JAX's collectives and lax.ppermute only.
A program may use at most 64 MiB of HBM per device.

```python
import math
import jax
import jax.numpy as jnp
import numpy as np
from jax import lax

C = 128
N = 768
NCHAIN = 8


def level_of(stream_key, shape, shards, least, high):
    def one(position, blocks):
        heights = jax.random.uniform(jax.random.fold_in(jax.random.fold_in(stream_key, 6), position), (blocks,), jnp.float32, least / len(shards), high / len(shards))
        return jnp.repeat(jnp.exp(heights), shape[position] // blocks).reshape((-1,) + (1,) * (len(shape) - position - 1))

    level = one(*shards[0])
    for cut in shards[1:]:
        level = level * one(*cut)
    return level


def profile(amount, total, bound, lean):
    weights = [(1 << 20) // math.isqrt(rank ** lean) + 1 for rank in range(2, amount + 1)]
    spare, holding = total - bound - (amount - 1), [1] * (amount - 1)
    while spare > 0:
        free = [i for i in range(amount - 1) if holding[i] < bound]
        mass, budget = sum([weights[i] for i in free]), spare
        for i in free:
            more = min(bound - holding[i], max(1, budget * weights[i] // mass), spare)
            holding[i] = holding[i] + more
            spare = spare - more
    return np.array([bound] + holding)


def uneven_parts(rng, count, total, most, skew):
    if count == 2:
        one = jax.random.randint(rng, (), max(1, total - most), min(most, total - 1) + 1)
        return jnp.stack([one, total - one])
    sizes = jnp.asarray(profile(count, total, most, skew), jnp.int32)
    pairs = (count - 1) // 2
    giver, sink = sizes[1:1 + 2 * pairs:2], sizes[2:2 + 2 * pairs:2]
    slack = jnp.minimum(giver - 1, most - sink)
    passed = jax.random.randint(jax.random.fold_in(rng, 1), (pairs,), 0, 1 << 20) % (slack + 1)
    sizes = sizes.at[1:1 + 2 * pairs:2].set(giver - passed).at[2:2 + 2 * pairs:2].set(sink + passed)
    return sizes[jax.random.permutation(jax.random.fold_in(rng, 2), count)]


def bell_draw(stream_key, shape, deviation, bound, cuts=(), held_as=jnp.bfloat16):
    array = deviation * jax.random.normal(stream_key, shape, jnp.float32)
    if cuts:
        array = array * level_of(stream_key, shape, cuts, -0.22, 0.18)
    return jnp.clip(array, -bound, bound).astype(held_as)


def setup_inputs(seed: int = 0) -> dict:
    key_of = jax.random.split(jax.random.key(seed), 7)
    return {
        "pair": bell_draw(key_of[0], (N, N, C), 1.0, 6.0, ((0, 16), (1, 8))),
        "chain_lengths": uneven_parts(key_of[1], NCHAIN, 3 * N // 4, N // NCHAIN, 1).astype(jnp.int32),
        "gains": jnp.clip(1.0 + 0.18 * jax.random.normal(key_of[2], (2, 2, C), jnp.float32), 0.1, 1.9),
        "biases": bell_draw(key_of[3], (2, 2, C), 0.5, 3.0, (), jnp.float32),
        "w_in": bell_draw(key_of[4], (2, C, 5 * C), C ** -0.5, 0.5),
        "w_out": bell_draw(key_of[5], (2, C, C), C ** -0.5, 0.5),
    }


def layer_norm(values, gain_vec, bias_vec):
    wide = values.astype(jnp.float32)
    average = lax.optimization_barrier(jnp.mean(wide, axis=-1, keepdims=True))
    centred = wide - average
    variance = lax.optimization_barrier(jnp.mean(centred * centred, axis=-1, keepdims=True))
    return centred * jax.lax.rsqrt(variance + 1e-05) * gain_vec + bias_vec

def live_mask(chain_lengths):
    slot_size = N // NCHAIN
    positions = jnp.arange(N, dtype=jnp.int32)
    live_length = chain_lengths[positions // slot_size]
    return (positions % slot_size < live_length).astype(jnp.float32)

def one_update(state, pmask, gain_pair, bias_pair, weights_in, weights_out, incoming):
    channels = state.shape[-1]
    normed = layer_norm(state, gain_pair[0], bias_pair[0]).astype(jnp.bfloat16)
    flat = normed.reshape(N * N, channels)

    def project(column_block):
        block = weights_in[:, column_block * channels:(column_block + 1) * channels]
        return jnp.dot(flat, block, preferred_element_type=jnp.float32).reshape(N, N, channels)
    left_edges = (pmask * jax.nn.sigmoid(project(1)) * project(0)).astype(jnp.bfloat16)
    right_edges = (pmask * jax.nn.sigmoid(project(3)) * project(2)).astype(jnp.bfloat16)
    left_wide = left_edges.astype(jnp.float32)
    right_wide = right_edges.astype(jnp.float32)
    if incoming:
        products = jnp.einsum('kic,kjc->ijc', left_wide, right_wide)
    else:
        products = jnp.einsum('ikc,jkc->ijc', left_wide, right_wide)
    products = products.astype(jnp.bfloat16)
    normed_out = layer_norm(products, gain_pair[1], bias_pair[1]).astype(jnp.bfloat16)
    mixed = jnp.dot(normed_out.reshape(N * N, channels), weights_out, preferred_element_type=jnp.float32).reshape(N, N, channels)
    gate_vals = jax.nn.sigmoid(project(4))
    return (state.astype(jnp.float32) + gate_vals * mixed).astype(jnp.bfloat16)

def reference(pair, chain_lengths, gains, biases, w_in, w_out):
    live = live_mask(chain_lengths)
    pmask = (live[:, None] * live[None, :])[:, :, None]
    state = pair
    for update_index in range(2):
        state = one_update(state, pmask, gains[update_index], biases[update_index], w_in[update_index], w_out[update_index], update_index == 1)
    return state
```

```python
import functools
import jax
import jax.numpy as jnp
from jax import lax
from jax.experimental import pallas as pl
from jax.experimental.pallas import tpu as pltpu
from jax.sharding import PartitionSpec as P

N = 768
NCHAIN = 8
C = 128
ROWS, COLS = 16, 8
TR, TC = N // ROWS, N // COLS
ILO, IHI, KHI, KLO = 4, 12, 3, 32
NQ = IHI * KHI
SA = 2 * NQ
SP = 40
BF, F32 = jnp.bfloat16, jnp.float32


def live_values(global_index, chain_lengths):
    slot_size = N // NCHAIN
    chain_index = global_index // slot_size
    offset = global_index % slot_size
    matches = chain_index[:, None] == jnp.arange(NCHAIN, dtype=jnp.int32)[None, :]
    live_length = jnp.sum(jnp.where(matches, chain_lengths[None, :], 0), axis=1)
    return (offset < live_length).astype(F32)


def sigmoid(x):
    return 0.5 * jnp.tanh(0.5 * x) + 0.5


def norm_rows(z, gain, bias):
    wide = z.astype(F32)
    mean = jnp.mean(wide, axis=1, keepdims=True)
    centred = wide - mean
    var = jnp.mean(centred * centred, axis=1, keepdims=True)
    return centred * lax.rsqrt(var + 1e-05) * gain + bias


def pre_kernel(z_ref, w_ref, gb_ref, mask_ref, out_ref, scr):
    gain = gb_ref[0:1, :]
    bias = gb_ref[1:2, :]

    def step(t, carry):
        for h in range(KHI):
            parts = []
            for e in range(2):
                z = z_ref[:, 2 * t + e, h * KLO:(h + 1) * KLO, :].reshape(C, C)
                parts.append(norm_rows(z, gain, bias).astype(BF))
            normed = jnp.concatenate(parts, axis=0)
            rows = [h * IHI + 2 * t + e for e in range(2)]
            mask = jnp.concatenate([mask_ref[pl.ds(r, 1), :] for r in rows], axis=1)
            for side in range(2):
                value, gate = (
                    lax.dot_general(
                        w_ref[(2 * side + k) * C:(2 * side + k + 1) * C, :], normed,
                        (((1,), (1,)), ((), ())), preferred_element_type=F32)
                    for k in range(2)
                )
                edges = mask * sigmoid(gate) * value
                for e in range(2):
                    row = h * 2 * IHI + side * IHI + 2 * t + e
                    scr[pl.ds(row, C, stride=SA), :] = edges[:, e * C:(e + 1) * C]
        return carry

    lax.fori_loop(0, IHI // 2, step, 0)

    def cast(s, carry):
        out_ref[s] = scr[pl.ds(pl.multiple_of(s * SA, 8), 2 * NQ), :].astype(BF)
        return carry

    lax.fori_loop(0, C, cast, 0, unroll=4)


def swap_blocks(x):
    lane = lax.broadcasted_iota(jnp.int32, x[0].shape, 1)
    low64 = lane < 64
    low32 = (lane % 64) < 32
    t = [None] * 4
    for b in range(2):
        t[b] = jnp.where(low64, x[b], pltpu.roll(x[b + 2], 64, 1))
        t[b + 2] = jnp.where(low64, pltpu.roll(x[b], 64, 1), x[b + 2])
    y = []
    for b in (0, 2):
        y.append(jnp.where(low32, t[b], pltpu.roll(t[b + 1], 32, 1)))
        y.append(jnp.where(low32, pltpu.roll(t[b], 96, 1), t[b + 1]))
    return y


def tri_kernel(in_ref, out_ref, ml, mr, mlb, mrb, tri, oscr, *, incoming):
    def gather(r, carry):
        for v in range(6):
            x = []
            for b in range(4):
                c, h = divmod(4 * v + b, KHI)
                whole = in_ref[r * COLS + c].astype(F32)
                x.append(whole[h * 24:(h + 1) * 24, :])
            y = swap_blocks(x)
            for a in range(4):
                rows, lanes = slice(a * IHI, (a + 1) * IHI), slice(v * C, (v + 1) * C)
                ml[r, rows, lanes] = y[a][0:IHI]
                mr[r, rows, lanes] = y[a][IHI:2 * IHI]
        return carry

    lax.fori_loop(0, ROWS, gather, 0)
    mlb[...] = ml[...].reshape(N, N).astype(BF)
    mrb[...] = mr[...].reshape(N, N).astype(BF)
    for m in range(2):
        cut = slice(m * 384, (m + 1) * 384)
        if incoming:
            block = lax.dot_general(
                mlb[:, cut], mrb[...], (((0,), (0,)), ((), ())), preferred_element_type=F32)
        else:
            block = lax.dot_general(
                mlb[cut, :], mrb[...], (((1,), (1,)), ((), ())), preferred_element_type=F32)
        tri[m * 8:(m + 1) * 8] = block.reshape(8, TR, N)

    def scatter(r, carry):
        for v in range(6):
            x = [tri[r, a * IHI:(a + 1) * IHI, v * C:(v + 1) * C] for a in range(4)]
            y = swap_blocks(x)
            for b in range(4):
                c, h = divmod(4 * v + b, KHI)
                oscr[r * COLS + c, h * IHI:(h + 1) * IHI, :] = y[b]
        return carry

    lax.fori_loop(0, ROWS, scatter, 0)

    def cast(s, carry):
        out_ref[s] = oscr[s].astype(BF)
        return carry

    lax.fori_loop(0, C, cast, 0, unroll=4)


def post_kernel(in_ref, z_ref, gate_ref, gb_ref, w_ref, out_ref, scr):
    gain = jnp.broadcast_to(gb_ref[:, 0:1], (C, C))
    bias = jnp.broadcast_to(gb_ref[:, 1:2], (C, C))

    def widen(s, carry):
        scr[pl.ds(pl.multiple_of(s * SP, 8), NQ), :] = in_ref[s].astype(F32)
        return carry

    lax.fori_loop(0, C, widen, 0, unroll=4)

    def step(t, carry):
        for h in range(KHI):
            x = scr[pl.ds(h * IHI + t, C, stride=SP), :]
            mean = jnp.mean(x, axis=0, keepdims=True)
            centred = x - mean
            var = jnp.mean(centred * centred, axis=0, keepdims=True)
            normed = (centred * lax.rsqrt(var + 1e-05) * gain + bias).astype(BF)
            mixed = lax.dot_general(
                normed, w_ref[...], (((0,), (0,)), ((), ())), preferred_element_type=F32)
            cut = slice(h * KLO, (h + 1) * KLO)
            z = z_ref[:, t, cut, :].reshape(C, C).astype(F32)
            gate = gate_ref[:, t, cut, :].reshape(C, C)
            out_ref[:, t, cut, :] = (z + gate * mixed).astype(BF).reshape(ILO, KLO, C)
        return carry

    lax.fori_loop(0, IHI, step, 0)


def body(pair, chain_lengths, gains, biases, w_in, w_out):
    axes = ("row", "col")
    row_live = live_values(lax.axis_index("row") * TR + jnp.arange(TR, dtype=jnp.int32), chain_lengths)
    col_live = live_values(lax.axis_index("col") * TC + jnp.arange(TC, dtype=jnp.int32), chain_lengths)
    mask = (
        row_live.reshape(ILO, IHI).T[None, :, :, None] * col_live.reshape(KHI, 1, 1, KLO)
    ).reshape(NQ, C)
    state = pair.reshape(ILO, IHI, TC, C)
    for u in range(2):
        w = w_in[u]
        w_t = w[:, :4 * C].T
        gb_in = jnp.stack([gains[u, 0], biases[u, 0]])
        factors = pl.pallas_call(
            pre_kernel,
            out_shape=jax.ShapeDtypeStruct((C, 2 * NQ, C), BF),
            scratch_shapes=[pltpu.VMEM((C * SA, C), F32)],
            name="pre",
        )(state, w_t, gb_in, mask)
        factors = lax.all_to_all(factors, axes, 0, 0, tiled=True)
        normed = norm_rows(state.reshape(-1, C), gains[u, 0], biases[u, 0]).astype(BF)
        gate = jax.nn.sigmoid(jnp.dot(normed, w[:, 4 * C:], preferred_element_type=F32))
        gate = gate.reshape(ILO, IHI, TC, C)
        products = pl.pallas_call(
            functools.partial(tri_kernel, incoming=u == 1),
            out_shape=jax.ShapeDtypeStruct((C, NQ, C), BF),
            scratch_shapes=[
                pltpu.VMEM((ROWS, TR, N), F32), pltpu.VMEM((ROWS, TR, N), F32),
                pltpu.VMEM((N, N), BF), pltpu.VMEM((N, N), BF),
                pltpu.VMEM((ROWS, TR, N), F32), pltpu.VMEM((C, NQ, C), F32),
            ],
            name="tri",
        )(factors)
        products = lax.all_to_all(products, axes, 0, 0, tiled=True)
        gb_out = jnp.stack([gains[u, 1], biases[u, 1]], axis=1)
        state = pl.pallas_call(
            post_kernel,
            out_shape=jax.ShapeDtypeStruct((ILO, IHI, TC, C), BF),
            scratch_shapes=[pltpu.VMEM((C * SP, C), F32)],
            name="post",
        )(products, state, gate, gb_out, w_out[u])
    return state.reshape(TR, TC, C)


def solution(mesh):
    placed = (P("row", "col", None), P(), P(), P(), P(), P())
    return jax.shard_map(
        body, mesh=mesh, in_specs=placed, out_specs=P("row", "col", None), check_vma=False
    )
```

```python
import functools
import jax
import jax.numpy as jnp
from jax import lax
from jax.experimental import pallas as pl
from jax.experimental.pallas import tpu as pltpu
from jax.sharding import PartitionSpec as P

N = 768
C = 128
ROWS, COLS = 16, 8
TR, TC = N // ROWS, N // COLS
KHI, KLO = 3, 32
NQ = 36
SA, SP = 72, 40
STORES = 8
BF, F32 = jnp.bfloat16, jnp.float32


def norm_rows(z, gain, bias):
    wide = z.astype(F32)
    mean = jnp.mean(wide, axis=1, keepdims=True)
    centred = wide - mean
    var = jnp.mean(centred * centred, axis=1, keepdims=True)
    return centred * lax.rsqrt(var + 1e-05) * gain + bias


def sigmoid(x):
    return 0.5 * jnp.tanh(0.5 * x) + 0.5


def pick(parts, odd, high):
    return jnp.where(high, jnp.where(odd, parts[3], parts[2]), jnp.where(odd, parts[1], parts[0]))


def swap_blocks(x):
    lane = lax.broadcasted_iota(jnp.int32, x[0].shape, 1)
    odd, high = (lane // 32) % 2 == 1, lane >= 64
    skew = [pick([x[(b + d) % 4] for b in range(4)], odd, high) for d in range(4)]
    turned = [skew[0]] + [pltpu.roll(skew[d], 32 * d, 1) for d in range(1, 4)]
    return [pick([turned[(b - a) % 4] for b in range(4)], odd, high) for a in range(4)]


def tri_kernel(in_ref, out_hbm, mlb, mrb, tri, stage, sems, *, incoming):
    top = lax.broadcasted_iota(jnp.int32, (8, C), 0) < 4

    def gather(r, carry):
        whole = [in_ref[r * COLS + c].astype(F32) for c in range(COLS)]
        for v in range(6):
            x = []
            for b in range(4):
                c, h = divmod(4 * v + b, KHI)
                x.append(whole[c][h * 24:(h + 1) * 24, :])
            y = swap_blocks(x)
            tail = [z[16:24] for z in y]
            left, right = [z[0:8] for z in y], [z[8:16] for z in y]
            for a in (0, 2):
                left.append(jnp.where(top, tail[a], pltpu.roll(tail[a + 1], 4, 0)))
                right.append(jnp.where(top, pltpu.roll(tail[a], 4, 0), tail[a + 1]))
            rows, lanes = pl.ds(pl.multiple_of(r * TR, TR), TR), slice(v * C, (v + 1) * C)
            mlb[rows, lanes] = jnp.concatenate(left, axis=0).astype(BF)
            mrb[rows, lanes] = jnp.concatenate(right, axis=0).astype(BF)
        return carry

    lax.fori_loop(0, ROWS, gather, 0, unroll=2)
    for m in range(2):
        cut = slice(m * 384, (m + 1) * 384)
        if incoming:
            tri[cut, :] = lax.dot_general(
                mlb[:, cut], mrb[...], (((0,), (0,)), ((), ())), preferred_element_type=F32)
        else:
            tri[cut, :] = lax.dot_general(
                mlb[cut, :], mrb[...], (((1,), (1,)), ((), ())), preferred_element_type=F32)

    def copy_out(r):
        dests = pl.ds(r * 2 * COLS, 2 * COLS)
        return pltpu.make_async_copy(stage.at[dests], out_hbm.at[dests], sems.at[r])

    def scatter(t, carry):
        rs = (2 * t, 2 * t + 1)
        base = [pl.multiple_of(r * TR, TR) for r in rs]
        main, tail = ([], []), []
        for v in range(6):
            lanes = slice(v * C, (v + 1) * C)
            for e in range(2):
                main[e].extend(swap_blocks([tri[pl.ds(base[e] + 8 * a, 8), lanes] for a in range(4)]))
            ends = []
            for a in (32, 40):
                p, q = (tri[pl.ds(base[e] + a, 8), lanes] for e in range(2))
                ends.append(jnp.where(top, p, pltpu.roll(q, 4, 0)))
                ends.append(jnp.where(top, pltpu.roll(p, 4, 0), q))
            tail += swap_blocks(ends)
        for c in range(COLS):
            j = tail[KHI * c:KHI * c + KHI]
            last = (
                [jnp.where(top, j[0], pltpu.roll(j[1], 4, 0)), j[2]],
                [jnp.where(top, pltpu.roll(j[0], 4, 0), j[1]), pltpu.roll(j[2], 4, 0)],
            )
            for e in range(2):
                block = jnp.concatenate(main[e][KHI * c:KHI * c + KHI] + last[e], axis=0)
                stage[rs[e] * COLS + c] = block.astype(BF)
        copy_out(t).start()
        return carry

    lax.fori_loop(0, ROWS // 2, scatter, 0)

    def finish(r, carry):
        copy_out(r).wait()
        return carry

    lax.fori_loop(0, ROWS // 2, finish, 0)


def place(g):
    h, part = g // 3, g % 3
    tail = part == 2
    row = jnp.where(tail, TR - 16, 4 * part)
    step = jnp.where(tail, 4, 8)
    factor_rows = [h * 24 + jnp.where(tail, 16 + 4 * side, 8 * side + 4 * part) for side in range(2)]
    product_row = jnp.where(tail, 24 + 4 * h, 8 * h + 4 * part)
    return h, row, step, factor_rows, product_row


def copies(src, dst, sems, cuts):
    return [pltpu.make_async_copy(src.at[k], dst.at[k], sems.at[n]) for n, k in enumerate(cuts)]


def column_cuts():
    return [(slice(None), pl.ds(h * KLO, KLO)) for h in range(KHI)]


def wait_column(g, *lists):
    for h in range(KHI):
        @pl.when(g == 3 * h)
        def _():
            for some in lists:
                some[h].wait()


def load_chunk(z, row, step, h):
    cut = pl.ds(pl.multiple_of(h * KLO, KLO), KLO)
    return jnp.concatenate([z[row + a * step, cut, :] for a in range(4)], axis=0)


def store_chunk(z, row, step, h, value):
    cut = pl.ds(pl.multiple_of(h * KLO, KLO), KLO)
    for a in range(4):
        z[row + a * step, cut, :] = value[a * KLO:(a + 1) * KLO]


def projector(chain, w, gains, biases, scr, u):
    row, col = lax.axis_index("row"), lax.axis_index("col")
    live_rows = chain[row // 2] - TR * (row % 2)
    live_cols = chain[col]
    gain, bias = gains[u, 0:1, :], biases[u, 0:1, :]
    w_t = [w[u, :, k * C:(k + 1) * C].T for k in range(4)]
    lane = lax.broadcasted_iota(jnp.int32, (1, C), 1)

    def project(chunks, h, first, step, factor_rows):
        lane_row, lane_col = lane // KLO * step + first, lane % KLO + h * KLO
        for half in range(2):
            es = (2 * half, 2 * half + 1)
            normed = jnp.concatenate([norm_rows(chunks[e], gain, bias).astype(BF) for e in es], axis=0)
            mask = jnp.concatenate(
                [((lane_row + e < live_rows) & (lane_col < live_cols)).astype(F32) for e in es], axis=1)
            for side in range(2):
                value, gate = (
                    lax.dot_general(
                        w_t[2 * side + k], normed, (((1,), (1,)), ((), ())), preferred_element_type=F32)
                    for k in range(2)
                )
                edges = mask * sigmoid(gate) * value
                for n, e in enumerate(es):
                    scr[pl.ds(factor_rows[side] + e, C, stride=SA), :] = edges[:, n * C:(n + 1) * C]

    return project


def send_factors(scr, stage, out, sems):
    per = C // STORES
    outs = copies(stage, out, sems, [pl.ds(n * per, per) for n in range(STORES)])

    def cast(s, carry):
        stage[s] = scr[pl.ds(pl.multiple_of(s * SA, 8), SA), :].astype(BF)
        return carry

    for n in range(STORES):
        lax.fori_loop(n * per, (n + 1) * per, cast, 0, unroll=4)
        outs[n].start()
    return outs


def pre_kernel(chain_hbm, z_hbm, w_hbm, gain_hbm, bias_hbm, out_hbm,
               chain, z, w, gains, biases, scr, stage, in_sems, z_sems, out_sems):
    small = [pltpu.make_async_copy(a, b, in_sems.at[n]) for n, (a, b) in enumerate(
        ((chain_hbm, chain), (w_hbm, w), (gain_hbm, gains), (bias_hbm, biases)))]
    z_in = copies(z_hbm, z, z_sems, column_cuts())
    for one in small + z_in:
        one.start()
    for one in small:
        one.wait()
    project = projector(chain, w, gains, biases, scr, 0)

    def step(g, carry):
        wait_column(g, z_in)
        h, row, gap, factor_rows, _ = place(g)
        project([load_chunk(z, row + e, gap, h) for e in range(4)], h, row, gap, factor_rows)
        return carry

    lax.fori_loop(0, 9, step, 0)
    for one in send_factors(scr, stage, out_hbm, out_sems):
        one.wait()


def post_parts(prod, z_hbm, gate_hbm, gains, biases, w_out, z, gate, wide, z_sems, gate_sems, u):
    z_in = copies(z_hbm, z, z_sems, column_cuts())
    gate_in = copies(gate_hbm, gate, gate_sems, column_cuts())
    for one in z_in + gate_in:
        one.start()
    gain = jnp.broadcast_to(gains[u, 1:2, :], (C, C)).T
    bias = jnp.broadcast_to(biases[u, 1:2, :], (C, C)).T

    def widen(s, carry):
        wide[pl.ds(pl.multiple_of(s * SP, 8), SP), :] = prod[s].astype(F32)
        return carry

    lax.fori_loop(0, C, widen, 0, unroll=4)

    def chunk(g, e):
        h, row, gap, _, product_row = place(g)
        x = wide[pl.ds(product_row + e, C, stride=SP), :]
        mean = jnp.mean(x, axis=0, keepdims=True)
        centred = x - mean
        var = jnp.mean(centred * centred, axis=0, keepdims=True)
        normed = (centred * lax.rsqrt(var + 1e-05) * gain + bias).astype(BF)
        mixed = lax.dot_general(
            normed, w_out[u], (((0,), (0,)), ((), ())), preferred_element_type=F32)
        old = load_chunk(z, row + e, gap, h).astype(F32)
        return (old + load_chunk(gate, row + e, gap, h) * mixed).astype(BF)

    return z_in, gate_in, chunk


def mid_kernel(chain, prod, z_hbm, gate_hbm, w, gains, biases, w_out, z_out_hbm, out_hbm,
               z, gate, wide, z_out, scr, stage, z_sems, gate_sems, zo_sems, out_sems):
    z_in, gate_in, chunk = post_parts(
        prod, z_hbm, gate_hbm, gains, biases, w_out, z, gate, wide, z_sems, gate_sems, 0)
    project = projector(chain, w, gains, biases, scr, 1)
    z_done = copies(z_out, z_out_hbm, zo_sems, column_cuts())

    def step(g, carry):
        wait_column(g, z_in, gate_in)
        h, row, gap, factor_rows, _ = place(g)
        new = [chunk(g, e) for e in range(4)]
        for e in range(4):
            store_chunk(z_out, row + e, gap, h, new[e])
        project(new, h, row, gap, factor_rows)
        for k in range(KHI):
            @pl.when(g == 3 * k + 2)
            def _():
                z_done[k].start()
        return carry

    lax.fori_loop(0, 9, step, 0)
    for one in send_factors(scr, stage, out_hbm, out_sems) + z_done:
        one.wait()


def post_kernel(prod, z_hbm, gate_hbm, gains, biases, w_out, z_out_hbm,
                z, gate, wide, z_out, z_sems, gate_sems, zo_sems):
    z_in, gate_in, chunk = post_parts(
        prod, z_hbm, gate_hbm, gains, biases, w_out, z, gate, wide, z_sems, gate_sems, 1)
    z_done = copies(z_out, z_out_hbm, zo_sems, column_cuts())

    def step(g, carry):
        wait_column(g, z_in, gate_in)
        h, row, gap, _, _ = place(g)
        for e in range(4):
            store_chunk(z_out, row + e, gap, h, chunk(g, e))
        for k in range(KHI):
            @pl.when(g == 3 * k + 2)
            def _():
                z_done[k].start()
        return carry

    lax.fori_loop(0, 9, step, 0)
    for one in z_done:
        one.wait()


HBM = pl.BlockSpec(memory_space=pltpu.HBM)
VMEM = pl.BlockSpec(memory_space=pltpu.VMEM)
SMEM = pl.BlockSpec(memory_space=pltpu.SMEM)
FACTORS, PRODUCTS, STATE = ((C, 2 * NQ, C), BF), ((C, SP, C), BF), ((TR, TC, C), BF)


def call(kernel, name, outs, scratch, sems, limit, in_specs):
    shapes = [pltpu.HBM(*o) for o in outs]
    run = pl.pallas_call(
        kernel,
        out_shape=shapes if len(shapes) > 1 else shapes[0],
        in_specs=in_specs,
        out_specs=[HBM] * len(shapes) if len(shapes) > 1 else HBM,
        scratch_shapes=list(scratch) + [pltpu.SemaphoreType.DMA((n,)) for n in sems],
        compiler_params=pltpu.CompilerParams(vmem_limit_bytes=limit << 20),
        name=name,
    )

    def placed(*args):
        return run(*(
            pltpu.with_memory_space_constraint(a, s.memory_space)
            if s is HBM or (s is VMEM and a.size > N * N) else a
            for a, s in zip(args, in_specs)
        ))

    return placed


def kernels():
    V = pltpu.VMEM
    send = [V((C * SA, C), F32), V(*FACTORS)]
    pre = call(
        pre_kernel, "pre", [FACTORS],
        [pltpu.SMEM((8,), jnp.int32), V(*STATE), V((2, C, 5 * C), BF), V((2, 2, C), F32), V((2, 2, C), F32)] + send,
        [4, KHI, STORES], 20, [HBM] * 5)
    tri = [
        call(
            functools.partial(tri_kernel, incoming=u == 1), "tri", [PRODUCTS],
            [V((N, N), BF), V((N, N), BF), V((N, N), F32), V(*PRODUCTS)], [ROWS // 2], 20, [VMEM])
        for u in range(2)
    ]
    take = [V(*STATE), V(STATE[0], F32), V((C * SP, C), F32), V(*STATE)]
    mid = call(
        mid_kernel, "mid", [STATE, FACTORS], take + send, [KHI, KHI, KHI, STORES], 26,
        [SMEM, VMEM] + [HBM] * 2 + [VMEM] * 4)
    post = call(
        post_kernel, "post", [STATE], take, [KHI, KHI, KHI], 16, [VMEM] + [HBM] * 2 + [VMEM] * 3)
    return pre, tri, mid, post


def output_gate(state, w_in, gains, biases, u):
    normed = norm_rows(state.reshape(-1, C), gains[u, 0], biases[u, 0]).astype(BF)
    gate = jax.nn.sigmoid(jnp.dot(normed, w_in[u, :, 4 * C:], preferred_element_type=F32))
    return gate.reshape(state.shape)


def body(pair, chain_lengths, gains, biases, w_in, w_out):
    def exchange(blocks):
        return lax.all_to_all(blocks, ("row", "col"), 0, 0, tiled=True)

    pre, tri, mid, post = kernels()
    factors = exchange(pre(chain_lengths, pair, w_in, gains, biases))
    gate = output_gate(pair, w_in, gains, biases, 0)
    products = exchange(tri[0](factors))
    state, factors = mid(chain_lengths, products, pair, gate, w_in, gains, biases, w_out)
    factors = exchange(factors)
    gate = output_gate(state, w_in, gains, biases, 1)
    products = exchange(tri[1](factors))
    return post(products, state, gate, gains, biases, w_out)


def solution(mesh):
    placed = (P("row", "col", None), P(), P(), P(), P(), P())
    return jax.shard_map(
        body, mesh=mesh, in_specs=placed, out_specs=P("row", "col", None), check_vma=False
    )
```

```python
import functools
import jax
import jax.numpy as jnp
from jax import lax
from jax.experimental import pallas as pl
from jax.experimental.pallas import tpu as pltpu
from jax.sharding import PartitionSpec as P

N = 768
C = 128
ROWS, COLS = 16, 8
TR, TC = N // ROWS, N // COLS
KHI, KLO = 3, 32
NQ = 36
SA, SP = 24, 40
BF, F32 = jnp.bfloat16, jnp.float32


def norm_rows(z, gain, bias):
    wide = z.astype(F32)
    mean = jnp.mean(wide, axis=1, keepdims=True)
    centred = wide - mean
    var = jnp.mean(centred * centred, axis=1, keepdims=True)
    return centred * lax.rsqrt(var + 1e-05) * gain + bias


def sigmoid(x):
    return 0.5 * jnp.tanh(0.5 * x) + 0.5


def pick(parts, odd, high):
    return jnp.where(high, jnp.where(odd, parts[3], parts[2]), jnp.where(odd, parts[1], parts[0]))


def swap_blocks(x):
    lane = lax.broadcasted_iota(jnp.int32, x[0].shape, 1)
    odd, high = (lane // 32) % 2 == 1, lane >= 64
    skew = [pick([x[(b + d) % 4] for b in range(4)], odd, high) for d in range(4)]
    turned = [skew[0]] + [pltpu.roll(skew[d], 32 * d, 1) for d in range(1, 4)]
    return [pick([turned[(b - a) % 4] for b in range(4)], odd, high) for a in range(4)]


def tri_kernel(in_ref, out_hbm, mlb, mrb, tri, stage, sems, *, incoming):
    top = lax.broadcasted_iota(jnp.int32, (8, C), 0) < 4

    def gather(r, carry):
        whole = [in_ref[r * COLS + c].astype(F32) for c in range(COLS)]
        for v in range(6):
            x = []
            for b in range(4):
                c, h = divmod(4 * v + b, KHI)
                x.append(whole[c][h * 24:(h + 1) * 24, :])
            y = swap_blocks(x)
            tail = [z[16:24] for z in y]
            left, right = [z[0:8] for z in y], [z[8:16] for z in y]
            for a in (0, 2):
                left.append(jnp.where(top, tail[a], pltpu.roll(tail[a + 1], 4, 0)))
                right.append(jnp.where(top, pltpu.roll(tail[a], 4, 0), tail[a + 1]))
            rows, lanes = pl.ds(pl.multiple_of(r * TR, TR), TR), slice(v * C, (v + 1) * C)
            mlb[rows, lanes] = jnp.concatenate(left, axis=0).astype(BF)
            mrb[rows, lanes] = jnp.concatenate(right, axis=0).astype(BF)
        return carry

    lax.fori_loop(0, ROWS, gather, 0, unroll=2)
    for m in range(2):
        cut = slice(m * 384, (m + 1) * 384)
        if incoming:
            tri[cut, :] = lax.dot_general(
                mlb[:, cut], mrb[...], (((0,), (0,)), ((), ())), preferred_element_type=F32)
        else:
            tri[cut, :] = lax.dot_general(
                mlb[cut, :], mrb[...], (((1,), (1,)), ((), ())), preferred_element_type=F32)

    def copy_out(r):
        dests = pl.ds(r * 2 * COLS, 2 * COLS)
        return pltpu.make_async_copy(stage.at[dests], out_hbm.at[dests], sems.at[r])

    def scatter(t, carry):
        rs = (2 * t, 2 * t + 1)
        base = [pl.multiple_of(r * TR, TR) for r in rs]
        main, tail = ([], []), []
        for v in range(6):
            lanes = slice(v * C, (v + 1) * C)
            for e in range(2):
                main[e].extend(swap_blocks([tri[pl.ds(base[e] + 8 * a, 8), lanes] for a in range(4)]))
            ends = []
            for a in (32, 40):
                p, q = (tri[pl.ds(base[e] + a, 8), lanes] for e in range(2))
                ends.append(jnp.where(top, p, pltpu.roll(q, 4, 0)))
                ends.append(jnp.where(top, pltpu.roll(p, 4, 0), q))
            tail += swap_blocks(ends)
        for c in range(COLS):
            j = tail[KHI * c:KHI * c + KHI]
            last = (
                [jnp.where(top, j[0], pltpu.roll(j[1], 4, 0)), j[2]],
                [jnp.where(top, pltpu.roll(j[0], 4, 0), j[1]), pltpu.roll(j[2], 4, 0)],
            )
            for e in range(2):
                block = jnp.concatenate(main[e][KHI * c:KHI * c + KHI] + last[e], axis=0)
                stage[rs[e] * COLS + c] = block.astype(BF)
        copy_out(t).start()
        return carry

    lax.fori_loop(0, ROWS // 2, scatter, 0)

    def finish(r, carry):
        copy_out(r).wait()
        return carry

    lax.fori_loop(0, ROWS // 2, finish, 0)


def place(part):
    if part == 2:
        return TR - 16, 4, (16, 20)
    return 4 * part, 8, (4 * part, 8 + 4 * part)


def product_row(part, h):
    return 24 + 4 * h if part == 2 else 8 * h + 4 * part


def column(ref, h):
    return ref.at[:, pl.ds(pl.multiple_of(h * KLO, KLO), KLO)]


def column_in(src, dst, sems, h):
    return pltpu.make_async_copy(column(src, h), column(dst, h), sems.at[h])


def load_chunk(z, row, step, h):
    cut = pl.ds(pl.multiple_of(h * KLO, KLO), KLO)
    return jnp.concatenate([z[row + a * step, cut, :] for a in range(4)], axis=0)


def store_chunk(z, row, step, h, value):
    cut = pl.ds(pl.multiple_of(h * KLO, KLO), KLO)
    for a in range(4):
        z[row + a * step, cut, :] = value[a * KLO:(a + 1) * KLO]


def projector(chain, w, gains, biases, scr, u):
    row, col = lax.axis_index("row"), lax.axis_index("col")
    live_rows = chain[row // 2] - TR * (row % 2)
    live_cols = chain[col]
    gain, bias = gains[u, 0:1, :], biases[u, 0:1, :]
    columns = w[u, :, 0:4 * C].T
    w_t = jnp.concatenate([
        columns[(2 * side + k) * C + d:(2 * side + k) * C + d + 16]
        for side in range(2) for d in range(0, C, 16) for k in range(2)
    ], axis=0)
    lane = lax.broadcasted_iota(jnp.int32, (1, C), 1)

    def project(chunks, h, part):
        first, step, factor_rows = place(part)
        lane_row, lane_col = lane // KLO * step + first, lane % KLO + h * KLO
        for half in range(2):
            es = (2 * half, 2 * half + 1)
            normed = jnp.concatenate([norm_rows(chunks[e], gain, bias).astype(BF) for e in es], axis=0)
            mask = jnp.concatenate(
                [((lane_row + e < live_rows) & (lane_col < live_cols)).astype(F32) for e in es], axis=1)
            every = lax.dot_general(
                w_t, normed, (((1,), (1,)), ((), ())), preferred_element_type=F32)
            for side in range(2):
                for d in range(0, C, 16):
                    at = 2 * (side * C + d)
                    value, gate = every[at:at + 16], every[at + 16:at + 32]
                    edges = mask * sigmoid(gate) * value
                    for n, e in enumerate(es):
                        rows = pl.ds(d * SA + factor_rows[side] + e, 16, stride=SA)
                        scr[rows, :] = edges[:, n * C:(n + 1) * C]

    return project


def factors_out(stage, out, sems, h):
    return pltpu.make_async_copy(stage.at[h], out.at[:, pl.ds(pl.multiple_of(h * SA, SA), SA)], sems.at[h])


def send_factors(scr, stage, out, sems, h):
    def cast(s, carry):
        stage[h, s] = scr[pl.ds(pl.multiple_of(s * SA, SA), SA), :].astype(BF)
        return carry

    lax.fori_loop(0, C, cast, 0, unroll=32)
    factors_out(stage, out, sems, h).start()


def each_column(step):
    def one(h, carry):
        step(h)
        return carry

    lax.fori_loop(0, KHI, one, 0)


def pre_kernel(chain_hbm, z_hbm, w_hbm, gain_hbm, bias_hbm, out_hbm,
               chain, z, w, gains, biases, scr, stage, in_sems, z_sems, out_sems):
    small = [pltpu.make_async_copy(a, b, in_sems.at[n]) for n, (a, b) in enumerate(
        ((chain_hbm, chain), (w_hbm, w), (gain_hbm, gains), (bias_hbm, biases)))]
    for one in small + [column_in(z_hbm, z, z_sems, h) for h in range(KHI)]:
        one.start()
    for one in small:
        one.wait()
    project = projector(chain, w, gains, biases, scr, 0)

    def step(h):
        column_in(z_hbm, z, z_sems, h).wait()
        for part in range(3):
            row, gap = place(part)[:2]
            project([load_chunk(z, row + e, gap, h) for e in range(4)], h, part)
        send_factors(scr, stage, out_hbm, out_sems, h)

    each_column(step)
    for h in range(KHI):
        factors_out(stage, out_hbm, out_sems, h).wait()


def post_parts(prod, z_hbm, gate_hbm, gains, biases, w_out, z, gate, wide, z_sems, gate_sems, u):
    for h in range(KHI):
        column_in(z_hbm, z, z_sems, h).start()
        column_in(gate_hbm, gate, gate_sems, h).start()
    gain = jnp.broadcast_to(gains[u, 1:2, :], (C, C)).T
    bias = jnp.broadcast_to(biases[u, 1:2, :], (C, C)).T

    def widen(s, carry):
        wide[pl.ds(pl.multiple_of(s * SP, 8), SP), :] = prod[s].astype(F32)
        return carry

    lax.fori_loop(0, C, widen, 0, unroll=8)

    def ready(h):
        column_in(z_hbm, z, z_sems, h).wait()
        column_in(gate_hbm, gate, gate_sems, h).wait()

    def chunk(h, part, e):
        row, gap = place(part)[:2]
        x = wide[pl.ds(product_row(part, h) + e, C, stride=SP), :]
        mean = jnp.mean(x, axis=0, keepdims=True)
        centred = x - mean
        var = jnp.mean(centred * centred, axis=0, keepdims=True)
        normed = (centred * lax.rsqrt(var + 1e-05) * gain + bias).astype(BF)
        mixed = lax.dot_general(
            normed, w_out[u], (((0,), (0,)), ((), ())), preferred_element_type=F32)
        old = load_chunk(z, row + e, gap, h).astype(F32)
        return (old + load_chunk(gate, row + e, gap, h) * mixed).astype(BF)

    return ready, chunk


def mid_kernel(chain, prod, z_hbm, gate_hbm, w, gains, biases, w_out, z_out_hbm, out_hbm,
               z, gate, wide, z_out, scr, stage, z_sems, gate_sems, zo_sems, out_sems):
    ready, chunk = post_parts(
        prod, z_hbm, gate_hbm, gains, biases, w_out, z, gate, wide, z_sems, gate_sems, 0)
    project = projector(chain, w, gains, biases, scr, 1)

    def step(h):
        ready(h)
        for part in range(3):
            row, gap = place(part)[:2]
            new = [chunk(h, part, e) for e in range(4)]
            for e in range(4):
                store_chunk(z_out, row + e, gap, h, new[e])
            project(new, h, part)
        column_in(z_out, z_out_hbm, zo_sems, h).start()
        send_factors(scr, stage, out_hbm, out_sems, h)

    each_column(step)
    for h in range(KHI):
        column_in(z_out, z_out_hbm, zo_sems, h).wait()
        factors_out(stage, out_hbm, out_sems, h).wait()


def post_kernel(prod, z_hbm, gate_hbm, gains, biases, w_out, z_out_hbm,
                z, gate, wide, z_out, z_sems, gate_sems, zo_sems):
    ready, chunk = post_parts(
        prod, z_hbm, gate_hbm, gains, biases, w_out, z, gate, wide, z_sems, gate_sems, 1)

    def step(h):
        ready(h)
        for part in range(3):
            row, gap = place(part)[:2]
            for e in range(4):
                store_chunk(z_out, row + e, gap, h, chunk(h, part, e))
        column_in(z_out, z_out_hbm, zo_sems, h).start()

    each_column(step)
    for h in range(KHI):
        column_in(z_out, z_out_hbm, zo_sems, h).wait()


HBM = pl.BlockSpec(memory_space=pltpu.HBM)
VMEM = pl.BlockSpec(memory_space=pltpu.VMEM)
SMEM = pl.BlockSpec(memory_space=pltpu.SMEM)
FACTORS, PRODUCTS, STATE = ((C, 2 * NQ, C), BF), ((C, SP, C), BF), ((TR, TC, C), BF)


def call(kernel, name, outs, scratch, sems, limit, in_specs):
    shapes = [pltpu.HBM(*o) for o in outs]
    run = pl.pallas_call(
        kernel,
        out_shape=shapes if len(shapes) > 1 else shapes[0],
        in_specs=in_specs,
        out_specs=[HBM] * len(shapes) if len(shapes) > 1 else HBM,
        scratch_shapes=list(scratch) + [pltpu.SemaphoreType.DMA((n,)) for n in sems],
        compiler_params=pltpu.CompilerParams(vmem_limit_bytes=limit << 20),
        name=name,
    )

    def placed(*args):
        return run(*(
            pltpu.with_memory_space_constraint(a, s.memory_space)
            if s is HBM or (s is VMEM and a.size > N * N) else a
            for a, s in zip(args, in_specs)
        ))

    return placed


def kernels():
    V = pltpu.VMEM
    send = [V((C * SA, C), F32), V((KHI, C, SA, C), BF)]
    pre = call(
        pre_kernel, "pre", [FACTORS],
        [pltpu.SMEM((8,), jnp.int32), V(*STATE), V((2, C, 5 * C), BF), V((2, 2, C), F32), V((2, 2, C), F32)] + send,
        [4, KHI, KHI], 20, [HBM] * 5)
    tri = [
        call(
            functools.partial(tri_kernel, incoming=u == 1), "tri", [PRODUCTS],
            [V((N, N), BF), V((N, N), BF), V((N, N), F32), V(*PRODUCTS)], [ROWS // 2], 20, [VMEM])
        for u in range(2)
    ]
    take = [V(*STATE), V(STATE[0], F32), V((C * SP, C), F32), V(*STATE)]
    mid = call(
        mid_kernel, "mid", [STATE, FACTORS], take + send, [KHI, KHI, KHI, KHI], 26,
        [SMEM, VMEM] + [HBM] * 2 + [VMEM] * 4)
    post = call(
        post_kernel, "post", [STATE], take, [KHI, KHI, KHI], 16, [VMEM] + [HBM] * 2 + [VMEM] * 3)
    return pre, tri, mid, post


def output_gate(state, w_in, gains, biases, u):
    normed = norm_rows(state.reshape(-1, C), gains[u, 0], biases[u, 0]).astype(BF)
    gate = jax.nn.sigmoid(jnp.dot(normed, w_in[u, :, 4 * C:], preferred_element_type=F32))
    return gate.reshape(state.shape)


def body(pair, chain_lengths, gains, biases, w_in, w_out):
    def exchange(blocks):
        return lax.all_to_all(blocks, ("row", "col"), 0, 0, tiled=True)

    pre, tri, mid, post = kernels()
    factors = exchange(pre(chain_lengths, pair, w_in, gains, biases))
    gate = output_gate(pair, w_in, gains, biases, 0)
    products = exchange(tri[0](factors))
    state, factors = mid(chain_lengths, products, pair, gate, w_in, gains, biases, w_out)
    factors = exchange(factors)
    gate = output_gate(state, w_in, gains, biases, 1)
    products = exchange(tri[1](factors))
    return post(products, state, gate, gains, biases, w_out)


def solution(mesh):
    placed = (P("row", "col", None), P(), P(), P(), P(), P())
    return jax.shard_map(
        body, mesh=mesh, in_specs=placed, out_specs=P("row", "col", None), check_vma=False
    )
```

```python
import functools
import jax
import jax.numpy as jnp
from jax import lax
from jax.experimental import pallas as pl
from jax.experimental.pallas import tpu as pltpu
from jax.sharding import PartitionSpec as P

N = 768
C = 128
ROWS, COLS = 16, 8
TR, TC = N // ROWS, N // COLS
KHI, KLO = 3, 32
NQ = 36
SA, SP = 24, 40
BF, F32 = jnp.bfloat16, jnp.float32


def norm_rows(z, gain, bias):
    wide = z.astype(F32)
    mean = jnp.mean(wide, axis=1, keepdims=True)
    centred = wide - mean
    var = jnp.mean(centred * centred, axis=1, keepdims=True)
    return centred * lax.rsqrt(var + 1e-05) * gain + bias


def sigmoid(x):
    return 0.5 * jnp.tanh(0.5 * x) + 0.5


def pick(parts, odd, high):
    return jnp.where(high, jnp.where(odd, parts[3], parts[2]), jnp.where(odd, parts[1], parts[0]))


def swap_blocks(x):
    lane = lax.broadcasted_iota(jnp.int32, x[0].shape, 1)
    odd, high = (lane // 32) % 2 == 1, lane >= 64
    skew = [pick([x[(b + d) % 4] for b in range(4)], odd, high) for d in range(4)]
    turned = [skew[0]] + [pltpu.roll(skew[d], 32 * d, 1) for d in range(1, 4)]
    return [pick([turned[(b - a) % 4] for b in range(4)], odd, high) for a in range(4)]


def tri_kernel(in_ref, out_hbm, mlb, mrb, tri, stage, sems, *, incoming):
    top = lax.broadcasted_iota(jnp.int32, (8, C), 0) < 4

    def gather(r, carry):
        whole = [in_ref[r * COLS + c].astype(F32) for c in range(COLS)]
        for v in range(6):
            x = []
            for b in range(4):
                c, h = divmod(4 * v + b, KHI)
                x.append(whole[c][h * 24:(h + 1) * 24, :])
            y = swap_blocks(x)
            tail = [z[16:24] for z in y]
            left, right = [z[0:8] for z in y], [z[8:16] for z in y]
            for a in (0, 2):
                left.append(jnp.where(top, tail[a], pltpu.roll(tail[a + 1], 4, 0)))
                right.append(jnp.where(top, pltpu.roll(tail[a], 4, 0), tail[a + 1]))
            rows, lanes = pl.ds(pl.multiple_of(r * TR, TR), TR), slice(v * C, (v + 1) * C)
            mlb[rows, lanes] = jnp.concatenate(left, axis=0).astype(BF)
            mrb[rows, lanes] = jnp.concatenate(right, axis=0).astype(BF)
        return carry

    lax.fori_loop(0, ROWS, gather, 0, unroll=4)
    for m in range(2):
        cut = slice(m * 384, (m + 1) * 384)
        if incoming:
            tri[cut, :] = lax.dot_general(
                mlb[:, cut], mrb[...], (((0,), (0,)), ((), ())), preferred_element_type=F32)
        else:
            tri[cut, :] = lax.dot_general(
                mlb[cut, :], mrb[...], (((1,), (1,)), ((), ())), preferred_element_type=F32)

    def copy_out(r):
        dests = pl.ds(r * 2 * COLS, 2 * COLS)
        return pltpu.make_async_copy(stage.at[dests], out_hbm.at[dests], sems.at[r])

    def scatter(t, carry):
        rs = (2 * t, 2 * t + 1)
        base = [pl.multiple_of(r * TR, TR) for r in rs]
        main, tail = ([], []), []
        for v in range(6):
            lanes = slice(v * C, (v + 1) * C)
            for e in range(2):
                main[e].extend(swap_blocks([tri[pl.ds(base[e] + 8 * a, 8), lanes] for a in range(4)]))
            ends = []
            for a in (32, 40):
                p, q = (tri[pl.ds(base[e] + a, 8), lanes] for e in range(2))
                ends.append(jnp.where(top, p, pltpu.roll(q, 4, 0)))
                ends.append(jnp.where(top, pltpu.roll(p, 4, 0), q))
            tail += swap_blocks(ends)
        for c in range(COLS):
            j = tail[KHI * c:KHI * c + KHI]
            last = (
                [jnp.where(top, j[0], pltpu.roll(j[1], 4, 0)), j[2]],
                [jnp.where(top, pltpu.roll(j[0], 4, 0), j[1]), pltpu.roll(j[2], 4, 0)],
            )
            for e in range(2):
                block = jnp.concatenate(main[e][KHI * c:KHI * c + KHI] + last[e], axis=0)
                stage[rs[e] * COLS + c] = block.astype(BF)
        copy_out(t).start()
        return carry

    lax.fori_loop(0, ROWS // 2, scatter, 0, unroll=2)

    def finish(r, carry):
        copy_out(r).wait()
        return carry

    lax.fori_loop(0, ROWS // 2, finish, 0)


def place(part):
    if part == 2:
        return TR - 16, 4, (16, 20)
    return 4 * part, 8, (4 * part, 8 + 4 * part)


def product_row(part, h):
    return 24 + 4 * h if part == 2 else 8 * h + 4 * part


def column(ref, h):
    return ref.at[:, pl.ds(pl.multiple_of(h * KLO, KLO), KLO)]


def column_in(src, dst, sems, h):
    return pltpu.make_async_copy(column(src, h), column(dst, h), sems.at[h])


def load_chunk(z, row, step, h):
    cut = pl.ds(pl.multiple_of(h * KLO, KLO), KLO)
    return jnp.concatenate([z[row + a * step, cut, :] for a in range(4)], axis=0)


def store_chunk(z, row, step, h, value):
    cut = pl.ds(pl.multiple_of(h * KLO, KLO), KLO)
    for a in range(4):
        z[row + a * step, cut, :] = value[a * KLO:(a + 1) * KLO]


def projector(chain, w, gains, biases, scr, u):
    row, col = lax.axis_index("row"), lax.axis_index("col")
    live_rows = chain[row // 2] - TR * (row % 2)
    live_cols = chain[col]
    gain, bias = gains[u, 0:1, :], biases[u, 0:1, :]
    columns = (w[u, :, 0:4 * C].astype(F32) * 0.5).T.astype(BF)
    w_t = jnp.concatenate([
        columns[(2 * side + k) * C + d:(2 * side + k) * C + d + 16]
        for side in range(2) for d in range(0, C, 16) for k in range(2)
    ], axis=0)
    lane = lax.broadcasted_iota(jnp.int32, (1, C), 1)

    def project(chunks, h, part):
        first, step, factor_rows = place(part)
        lane_row, lane_col = lane // KLO * step + first, lane % KLO + h * KLO
        for half in range(2):
            es = (2 * half, 2 * half + 1)
            normed = jnp.concatenate([norm_rows(chunks[e], gain, bias).astype(BF) for e in es], axis=0)
            mask = jnp.concatenate(
                [((lane_row + e < live_rows) & (lane_col < live_cols)).astype(F32) for e in es], axis=1)
            every = lax.dot_general(
                w_t, normed, (((1,), (1,)), ((), ())), preferred_element_type=F32)
            for side in range(2):
                for d in range(0, C, 16):
                    at = 2 * (side * C + d)
                    value, gate = every[at:at + 16], every[at + 16:at + 32]
                    edges = mask * (value * jnp.tanh(gate) + value)
                    for n, e in enumerate(es):
                        rows = pl.ds(d * SA + factor_rows[side] + e, 16, stride=SA)
                        scr[rows, :] = edges[:, n * C:(n + 1) * C]

    return project


def factors_out(stage, out, sems, h):
    return pltpu.make_async_copy(stage.at[h], out.at[:, pl.ds(pl.multiple_of(h * SA, SA), SA)], sems.at[h])


def send_factors(scr, stage, out, sems, h):
    def cast(s, carry):
        stage[h, s] = scr[pl.ds(pl.multiple_of(s * SA, SA), SA), :].astype(BF)
        return carry

    lax.fori_loop(0, C, cast, 0, unroll=32)
    factors_out(stage, out, sems, h).start()


def each_column(step):
    def one(h, carry):
        step(h)
        return carry

    lax.fori_loop(0, KHI, one, 0)


def pre_kernel(chain_hbm, z_hbm, w_hbm, gain_hbm, bias_hbm, out_hbm,
               chain, z, w, gains, biases, scr, stage, in_sems, z_sems, out_sems):
    small = [pltpu.make_async_copy(a, b, in_sems.at[n]) for n, (a, b) in enumerate(
        ((chain_hbm, chain), (w_hbm, w), (gain_hbm, gains), (bias_hbm, biases)))]
    for one in small + [column_in(z_hbm, z, z_sems, h) for h in range(KHI)]:
        one.start()
    for one in small:
        one.wait()
    project = projector(chain, w, gains, biases, scr, 0)

    def step(h):
        column_in(z_hbm, z, z_sems, h).wait()
        for part in range(3):
            row, gap = place(part)[:2]
            project([load_chunk(z, row + e, gap, h) for e in range(4)], h, part)
        send_factors(scr, stage, out_hbm, out_sems, h)

    each_column(step)
    for h in range(KHI):
        factors_out(stage, out_hbm, out_sems, h).wait()


def post_parts(prod, z_hbm, gate_hbm, gains, biases, w_out, z, gate, wide, z_sems, gate_sems, u):
    for h in range(KHI):
        column_in(z_hbm, z, z_sems, h).start()
        column_in(gate_hbm, gate, gate_sems, h).start()
    gain = jnp.broadcast_to(gains[u, 1:2, :], (C, C)).T
    bias = jnp.broadcast_to(biases[u, 1:2, :], (C, C)).T

    def widen(s, carry):
        wide[pl.ds(pl.multiple_of(s * SP, 8), SP), :] = prod[s].astype(F32)
        return carry

    lax.fori_loop(0, C, widen, 0, unroll=32)

    def ready(h):
        column_in(z_hbm, z, z_sems, h).wait()
        column_in(gate_hbm, gate, gate_sems, h).wait()

    def chunk(h, part, e):
        row, gap = place(part)[:2]
        x = wide[pl.ds(product_row(part, h) + e, C, stride=SP), :]
        mean = jnp.mean(x, axis=0, keepdims=True)
        centred = x - mean
        var = jnp.mean(centred * centred, axis=0, keepdims=True)
        normed = (centred * lax.rsqrt(var + 1e-05) * gain + bias).astype(BF)
        mixed = lax.dot_general(
            normed, w_out[u], (((0,), (0,)), ((), ())), preferred_element_type=F32)
        old = load_chunk(z, row + e, gap, h).astype(F32)
        return (old + load_chunk(gate, row + e, gap, h) * mixed).astype(BF)

    return ready, chunk


def mid_kernel(chain, prod, z_hbm, gate_hbm, w, gains, biases, w_out, z_out_hbm, out_hbm,
               z, gate, wide, z_out, scr, stage, z_sems, gate_sems, zo_sems, out_sems):
    ready, chunk = post_parts(
        prod, z_hbm, gate_hbm, gains, biases, w_out, z, gate, wide, z_sems, gate_sems, 0)
    project = projector(chain, w, gains, biases, scr, 1)

    def update(h):
        ready(h)
        for part in range(3):
            row, gap = place(part)[:2]
            for e in range(4):
                store_chunk(z_out, row + e, gap, h, chunk(h, part, e))
        column_in(z_out, z_out_hbm, zo_sems, h).start()

    def step(h):
        for part in range(3):
            row, gap = place(part)[:2]
            project([load_chunk(z_out, row + e, gap, h) for e in range(4)], h, part)
        send_factors(scr, stage, out_hbm, out_sems, h)

    each_column(update)
    each_column(step)
    for h in range(KHI):
        column_in(z_out, z_out_hbm, zo_sems, h).wait()
        factors_out(stage, out_hbm, out_sems, h).wait()


def post_kernel(prod, z_hbm, gate_hbm, gains, biases, w_out, z_out_hbm,
                z, gate, wide, z_out, z_sems, gate_sems, zo_sems):
    ready, chunk = post_parts(
        prod, z_hbm, gate_hbm, gains, biases, w_out, z, gate, wide, z_sems, gate_sems, 1)

    def step(h):
        ready(h)
        for part in range(3):
            row, gap = place(part)[:2]
            for e in range(4):
                store_chunk(z_out, row + e, gap, h, chunk(h, part, e))
        column_in(z_out, z_out_hbm, zo_sems, h).start()

    each_column(step)
    for h in range(KHI):
        column_in(z_out, z_out_hbm, zo_sems, h).wait()


HBM = pl.BlockSpec(memory_space=pltpu.HBM)
VMEM = pl.BlockSpec(memory_space=pltpu.VMEM)
SMEM = pl.BlockSpec(memory_space=pltpu.SMEM)
FACTORS, PRODUCTS, STATE = ((C, 2 * NQ, C), BF), ((C, SP, C), BF), ((TR, TC, C), BF)


def call(kernel, name, outs, scratch, sems, limit, in_specs):
    shapes = [pltpu.HBM(*o) for o in outs]
    run = pl.pallas_call(
        kernel,
        out_shape=shapes if len(shapes) > 1 else shapes[0],
        in_specs=in_specs,
        out_specs=[HBM] * len(shapes) if len(shapes) > 1 else HBM,
        scratch_shapes=list(scratch) + [pltpu.SemaphoreType.DMA((n,)) for n in sems],
        compiler_params=pltpu.CompilerParams(vmem_limit_bytes=limit << 20),
        name=name,
    )

    def placed(*args):
        return run(*(
            pltpu.with_memory_space_constraint(a, s.memory_space)
            if s is HBM or (s is VMEM and a.size > N * N) else a
            for a, s in zip(args, in_specs)
        ))

    return placed


def kernels():
    V = pltpu.VMEM
    send = [V((C * SA, C), F32), V((KHI, C, SA, C), BF)]
    pre = call(
        pre_kernel, "pre", [FACTORS],
        [pltpu.SMEM((8,), jnp.int32), V(*STATE), V((2, C, 5 * C), BF), V((2, 2, C), F32), V((2, 2, C), F32)] + send,
        [4, KHI, KHI], 20, [HBM] * 5)
    tri = [
        call(
            functools.partial(tri_kernel, incoming=u == 1), "tri", [PRODUCTS],
            [V((N, N), BF), V((N, N), BF), V((N, N), F32), V(*PRODUCTS)], [ROWS // 2], 20, [VMEM])
        for u in range(2)
    ]
    take = [V(*STATE), V(STATE[0], F32), V((C * SP, C), F32), V(*STATE)]
    mid = call(
        mid_kernel, "mid", [STATE, FACTORS], take + send, [KHI, KHI, KHI, KHI], 26,
        [SMEM, VMEM] + [HBM] * 2 + [VMEM] * 4)
    post = call(
        post_kernel, "post", [STATE], take, [KHI, KHI, KHI], 16, [VMEM] + [HBM] * 2 + [VMEM] * 3)
    return pre, tri, mid, post


def output_gate(state, w_in, gains, biases, u):
    normed = norm_rows(state.reshape(-1, C), gains[u, 0], biases[u, 0]).astype(BF)
    gate = jax.nn.sigmoid(jnp.dot(normed, w_in[u, :, 4 * C:], preferred_element_type=F32))
    return gate.reshape(state.shape)


def body(pair, chain_lengths, gains, biases, w_in, w_out):
    def exchange(blocks):
        return lax.all_to_all(blocks, ("row", "col"), 0, 0, tiled=True)

    pre, tri, mid, post = kernels()
    factors = exchange(pre(chain_lengths, pair, w_in, gains, biases))
    gate = output_gate(pair, w_in, gains, biases, 0)
    products = exchange(tri[0](factors))
    state, factors = mid(chain_lengths, products, pair, gate, w_in, gains, biases, w_out)
    factors = exchange(factors)
    gate = output_gate(state, w_in, gains, biases, 1)
    products = exchange(tri[1](factors))
    return post(products, state, gate, gains, biases, w_out)


def solution(mesh):
    placed = (P("row", "col", None), P(), P(), P(), P(), P())
    return jax.shard_map(
        body, mesh=mesh, in_specs=placed, out_specs=P("row", "col", None), check_vma=False
    )
```

```python
import functools
import jax
import jax.numpy as jnp
from jax import lax
from jax.experimental import pallas as pl
from jax.experimental.pallas import tpu as pltpu
from jax.sharding import PartitionSpec as P

N = 768
C = 128
ROWS, COLS = 16, 8
TR, TC = N // ROWS, N // COLS
KHI, KLO = 3, 32
NQ = 36
SA, SP = 24, 40
PARTS = 2
BF, F32 = jnp.bfloat16, jnp.float32


def norm_rows(z, gain, bias):
    wide = z.astype(F32)
    mean = jnp.mean(wide, axis=1, keepdims=True)
    centred = wide - mean
    var = jnp.mean(centred * centred, axis=1, keepdims=True)
    return centred * lax.rsqrt(var + 1e-05) * gain + bias


def sigmoid(x):
    return 0.5 * jnp.tanh(0.5 * x) + 0.5


def pick(parts, odd, high):
    return jnp.where(high, jnp.where(odd, parts[3], parts[2]), jnp.where(odd, parts[1], parts[0]))


def swap_blocks(x):
    lane = lax.broadcasted_iota(jnp.int32, x[0].shape, 1)
    odd, high = (lane // 32) % 2 == 1, lane >= 64
    skew = [pick([x[(b + d) % 4] for b in range(4)], odd, high) for d in range(4)]
    turned = [skew[0]] + [pltpu.roll(skew[d], 32 * d, 1) for d in range(1, 4)]
    return [pick([turned[(b - a) % 4] for b in range(4)], odd, high) for a in range(4)]


def tri_kernel(in_ref, out_hbm, mlb, mrb, tri, stage, sems, *, incoming):
    top = lax.broadcasted_iota(jnp.int32, (8, C), 0) < 4

    def gather(r, carry):
        whole = [in_ref[r * COLS + c].astype(F32) for c in range(COLS)]
        for v in range(6):
            x = []
            for b in range(4):
                c, h = divmod(4 * v + b, KHI)
                x.append(whole[c][h * 24:(h + 1) * 24, :])
            y = swap_blocks(x)
            tail = [z[16:24] for z in y]
            left, right = [z[0:8] for z in y], [z[8:16] for z in y]
            for a in (0, 2):
                left.append(jnp.where(top, tail[a], pltpu.roll(tail[a + 1], 4, 0)))
                right.append(jnp.where(top, pltpu.roll(tail[a], 4, 0), tail[a + 1]))
            rows, lanes = pl.ds(pl.multiple_of(r * TR, TR), TR), slice(v * C, (v + 1) * C)
            mlb[rows, lanes] = jnp.concatenate(left, axis=0).astype(BF)
            mrb[rows, lanes] = jnp.concatenate(right, axis=0).astype(BF)
        return carry

    lax.fori_loop(0, ROWS, gather, 0, unroll=4)
    for m in range(2):
        cut = slice(m * 384, (m + 1) * 384)
        if incoming:
            tri[cut, :] = lax.dot_general(
                mlb[:, cut], mrb[...], (((0,), (0,)), ((), ())), preferred_element_type=F32)
        else:
            tri[cut, :] = lax.dot_general(
                mlb[cut, :], mrb[...], (((1,), (1,)), ((), ())), preferred_element_type=F32)

    def copy_out(r):
        dests = pl.ds(r * 2 * COLS, 2 * COLS)
        return pltpu.make_async_copy(stage.at[dests], out_hbm.at[dests], sems.at[r])

    def scatter(t, carry):
        rs = (2 * t, 2 * t + 1)
        base = [pl.multiple_of(r * TR, TR) for r in rs]
        main, tail = ([], []), []
        for v in range(6):
            lanes = slice(v * C, (v + 1) * C)
            for e in range(2):
                main[e].extend(swap_blocks([tri[pl.ds(base[e] + 8 * a, 8), lanes] for a in range(4)]))
            ends = []
            for a in (32, 40):
                p, q = (tri[pl.ds(base[e] + a, 8), lanes] for e in range(2))
                ends.append(jnp.where(top, p, pltpu.roll(q, 4, 0)))
                ends.append(jnp.where(top, pltpu.roll(p, 4, 0), q))
            tail += swap_blocks(ends)
        for c in range(COLS):
            j = tail[KHI * c:KHI * c + KHI]
            last = (
                [jnp.where(top, j[0], pltpu.roll(j[1], 4, 0)), j[2]],
                [jnp.where(top, pltpu.roll(j[0], 4, 0), j[1]), pltpu.roll(j[2], 4, 0)],
            )
            for e in range(2):
                block = jnp.concatenate(main[e][KHI * c:KHI * c + KHI] + last[e], axis=0)
                stage[rs[e] * COLS + c] = block.astype(BF)
        copy_out(t).start()
        return carry

    lax.fori_loop(0, ROWS // 2, scatter, 0, unroll=2)

    def finish(r, carry):
        copy_out(r).wait()
        return carry

    lax.fori_loop(0, ROWS // 2, finish, 0)


def place(part):
    if part == 2:
        return TR - 16, 4, (16, 20)
    return 4 * part, 8, (4 * part, 8 + 4 * part)


def product_row(part, h):
    return 24 + 4 * h if part == 2 else 8 * h + 4 * part


def column(ref, h):
    return ref.at[:, pl.ds(pl.multiple_of(h * KLO, KLO), KLO)]


def column_in(src, dst, sems, h):
    return pltpu.make_async_copy(column(src, h), column(dst, h), sems.at[h])


def load_chunk(z, row, step, h):
    cut = pl.ds(pl.multiple_of(h * KLO, KLO), KLO)
    return jnp.concatenate([z[row + a * step, cut, :] for a in range(4)], axis=0)


def store_chunk(z, row, step, h, value):
    cut = pl.ds(pl.multiple_of(h * KLO, KLO), KLO)
    for a in range(4):
        z[row + a * step, cut, :] = value[a * KLO:(a + 1) * KLO]


def projector(chain, w, gains, biases, scr, u):
    row, col = lax.axis_index("row"), lax.axis_index("col")
    live_rows = chain[row // 2] - TR * (row % 2)
    live_cols = chain[col]
    gain, bias = gains[u, 0:1, :], biases[u, 0:1, :]
    columns = (w[u, :, 0:4 * C].astype(F32) * 0.5).T.astype(BF)
    w_t = jnp.concatenate([
        columns[(2 * side + k) * C + d:(2 * side + k) * C + d + 16]
        for side in range(2) for d in range(0, C, 16) for k in range(2)
    ], axis=0)
    lane = lax.broadcasted_iota(jnp.int32, (1, C), 1)

    def project(chunks, h, part):
        first, step, factor_rows = place(part)
        lane_row, lane_col = lane // KLO * step + first, lane % KLO + h * KLO
        for half in range(2):
            es = (2 * half, 2 * half + 1)
            normed = jnp.concatenate([norm_rows(chunks[e], gain, bias).astype(BF) for e in es], axis=0)
            mask = jnp.concatenate(
                [((lane_row + e < live_rows) & (lane_col < live_cols)).astype(F32) for e in es], axis=1)
            every = lax.dot_general(
                w_t, normed, (((1,), (1,)), ((), ())), preferred_element_type=F32)
            for side in range(2):
                for d in range(0, C, 16):
                    at = 2 * (side * C + d)
                    value, gate = every[at:at + 16], every[at + 16:at + 32]
                    edges = mask * (value * jnp.tanh(gate) + value)
                    for n, e in enumerate(es):
                        rows = pl.ds(d * SA + factor_rows[side] + e, 16, stride=SA)
                        scr[rows, :] = edges[:, n * C:(n + 1) * C]

    return project


def factors_out(stage, out, sems, h, part):
    dests = pl.ds(part * (C // PARTS), C // PARTS)
    return pltpu.make_async_copy(
        stage.at[h, dests], out.at[dests, pl.ds(pl.multiple_of(h * SA, SA), SA)], sems.at[h, part])


def send_factors(scr, stage, out, sems, h):
    def cast(s, carry):
        stage[h, s] = scr[pl.ds(pl.multiple_of(s * SA, SA), SA), :].astype(BF)
        return carry

    for part in range(PARTS):
        lax.fori_loop(part * (C // PARTS), (part + 1) * (C // PARTS), cast, 0, unroll=32)
        factors_out(stage, out, sems, h, part).start()


def each_column(step):
    def one(h, carry):
        step(h)
        return carry

    lax.fori_loop(0, KHI, one, 0, unroll=True)


def pre_kernel(chain_hbm, z_hbm, w_hbm, gain_hbm, bias_hbm, out_hbm,
               chain, z, w, gains, biases, scr, stage, in_sems, z_sems, out_sems):
    small = [pltpu.make_async_copy(a, b, in_sems.at[n]) for n, (a, b) in enumerate(
        ((chain_hbm, chain), (w_hbm, w), (gain_hbm, gains), (bias_hbm, biases)))]
    for one in small + [column_in(z_hbm, z, z_sems, h) for h in range(KHI)]:
        one.start()
    for one in small:
        one.wait()
    project = projector(chain, w, gains, biases, scr, 0)

    def step(h):
        column_in(z_hbm, z, z_sems, h).wait()
        for part in range(3):
            row, gap = place(part)[:2]
            project([load_chunk(z, row + e, gap, h) for e in range(4)], h, part)
        send_factors(scr, stage, out_hbm, out_sems, h)

    each_column(step)
    for h in range(KHI):
        for part in range(PARTS):
            factors_out(stage, out_hbm, out_sems, h, part).wait()


def post_parts(prod, z_hbm, gate_hbm, gains, biases, w_out, z, gate, wide, normed, z_sems, gate_sems, u):
    for h in range(KHI):
        column_in(z_hbm, z, z_sems, h).start()
        column_in(gate_hbm, gate, gate_sems, h).start()
    gain = jnp.broadcast_to(gains[u, 1:2, :], (C, C)).T
    bias = jnp.broadcast_to(biases[u, 1:2, :], (C, C)).T

    def widen(s, carry):
        wide[pl.ds(pl.multiple_of(s * SP, 8), SP), :] = prod[s].astype(F32)
        return carry

    lax.fori_loop(0, C, widen, 0, unroll=32)

    def normalise(h):
        for part in range(3):
            for e in range(4):
                x = wide[pl.ds(product_row(part, h) + e, C, stride=SP), :]
                mean = jnp.mean(x, axis=0, keepdims=True)
                centred = x - mean
                var = jnp.mean(centred * centred, axis=0, keepdims=True)
                normed[h, 4 * part + e] = (centred * lax.rsqrt(var + 1e-05) * gain + bias).astype(BF)

    each_column(normalise)

    def update(z_out, h):
        column_in(z_hbm, z, z_sems, h).wait()
        column_in(gate_hbm, gate, gate_sems, h).wait()
        for part in range(3):
            row, gap = place(part)[:2]
            for e in range(4):
                mixed = lax.dot_general(
                    normed[h, 4 * part + e], w_out[u], (((0,), (0,)), ((), ())), preferred_element_type=F32)
                old = load_chunk(z, row + e, gap, h).astype(F32)
                new = old + load_chunk(gate, row + e, gap, h) * mixed
                store_chunk(z_out, row + e, gap, h, new.astype(BF))

    return update


def mid_kernel(chain, prod, z_hbm, gate_hbm, w, gains, biases, w_out, z_out_hbm, out_hbm,
               z, gate, wide, normed, z_out, scr, stage, z_sems, gate_sems, zo_sems, out_sems):
    update = post_parts(
        prod, z_hbm, gate_hbm, gains, biases, w_out, z, gate, wide, normed, z_sems, gate_sems, 0)
    project = projector(chain, w, gains, biases, scr, 1)

    def renew(h):
        update(z_out, h)
        column_in(z_out, z_out_hbm, zo_sems, h).start()

    def step(h):
        for part in range(3):
            row, gap = place(part)[:2]
            project([load_chunk(z_out, row + e, gap, h) for e in range(4)], h, part)
        send_factors(scr, stage, out_hbm, out_sems, h)

    each_column(renew)
    each_column(step)
    for h in range(KHI):
        column_in(z_out, z_out_hbm, zo_sems, h).wait()
        for part in range(PARTS):
            factors_out(stage, out_hbm, out_sems, h, part).wait()


def post_kernel(prod, z_hbm, gate_hbm, gains, biases, w_out, z_out_hbm,
                z, gate, wide, normed, z_out, z_sems, gate_sems, zo_sems):
    update = post_parts(
        prod, z_hbm, gate_hbm, gains, biases, w_out, z, gate, wide, normed, z_sems, gate_sems, 1)

    def step(h):
        update(z_out, h)
        column_in(z_out, z_out_hbm, zo_sems, h).start()

    each_column(step)
    for h in range(KHI):
        column_in(z_out, z_out_hbm, zo_sems, h).wait()


HBM = pl.BlockSpec(memory_space=pltpu.HBM)
VMEM = pl.BlockSpec(memory_space=pltpu.VMEM)
SMEM = pl.BlockSpec(memory_space=pltpu.SMEM)
FACTORS, PRODUCTS, STATE = ((C, 2 * NQ, C), BF), ((C, SP, C), BF), ((TR, TC, C), BF)


def call(kernel, name, outs, scratch, sems, limit, in_specs):
    shapes = [pltpu.HBM(*o) for o in outs]
    run = pl.pallas_call(
        kernel,
        out_shape=shapes if len(shapes) > 1 else shapes[0],
        in_specs=in_specs,
        out_specs=[HBM] * len(shapes) if len(shapes) > 1 else HBM,
        scratch_shapes=list(scratch) + [pltpu.SemaphoreType.DMA(n if isinstance(n, tuple) else (n,)) for n in sems],
        compiler_params=pltpu.CompilerParams(vmem_limit_bytes=limit << 20),
        name=name,
    )

    def placed(*args):
        return run(*(
            pltpu.with_memory_space_constraint(a, s.memory_space)
            if s is HBM or (s is VMEM and a.size > N * N) else a
            for a, s in zip(args, in_specs)
        ))

    return placed


def kernels():
    V = pltpu.VMEM
    send = [V((C * SA, C), F32), V((KHI, C, SA, C), BF)]
    pre = call(
        pre_kernel, "pre", [FACTORS],
        [pltpu.SMEM((8,), jnp.int32), V(*STATE), V((2, C, 5 * C), BF), V((2, 2, C), F32), V((2, 2, C), F32)] + send,
        [4, KHI, (KHI, PARTS)], 20, [HBM] * 5)
    tri = [
        call(
            functools.partial(tri_kernel, incoming=u == 1), "tri", [PRODUCTS],
            [V((N, N), BF), V((N, N), BF), V((N, N), F32), V(*PRODUCTS)], [ROWS // 2], 20, [VMEM])
        for u in range(2)
    ]
    take = [V(*STATE), V(STATE[0], F32), V((C * SP, C), F32), V((KHI, 12, C, C), BF), V(*STATE)]
    mid = call(
        mid_kernel, "mid", [STATE, FACTORS], take + send, [KHI, KHI, KHI, (KHI, PARTS)], 26,
        [SMEM, VMEM] + [HBM] * 2 + [VMEM] * 4)
    post = call(
        post_kernel, "post", [STATE], take, [KHI, KHI, KHI], 16, [VMEM] + [HBM] * 2 + [VMEM] * 3)
    return pre, tri, mid, post


def output_gate(state, w_in, gains, biases, u):
    normed = norm_rows(state.reshape(-1, C), gains[u, 0], biases[u, 0]).astype(BF)
    gate = jax.nn.sigmoid(jnp.dot(normed, w_in[u, :, 4 * C:], preferred_element_type=F32))
    return gate.reshape(state.shape)


def body(pair, chain_lengths, gains, biases, w_in, w_out):
    def exchange(blocks):
        return lax.all_to_all(blocks, ("row", "col"), 0, 0, tiled=True)

    pre, tri, mid, post = kernels()
    factors = exchange(pre(chain_lengths, pair, w_in, gains, biases))
    gate = output_gate(pair, w_in, gains, biases, 0)
    products = exchange(tri[0](factors))
    state, factors = mid(chain_lengths, products, pair, gate, w_in, gains, biases, w_out)
    factors = exchange(factors)
    gate = output_gate(state, w_in, gains, biases, 1)
    products = exchange(tri[1](factors))
    return post(products, state, gate, gains, biases, w_out)


def solution(mesh):
    placed = (P("row", "col", None), P(), P(), P(), P(), P())
    return jax.shard_map(
        body, mesh=mesh, in_specs=placed, out_specs=P("row", "col", None), check_vma=False
    )
```

```python
import functools
import jax
import jax.numpy as jnp
from jax import lax
from jax.experimental import pallas as pl
from jax.experimental.pallas import tpu as pltpu
from jax.sharding import PartitionSpec as P

N = 768
C = 128
ROWS, COLS = 16, 8
TR, TC = N // ROWS, N // COLS
KHI, KLO = 3, 32
NQ = 36
SA, SP = 24, 40
PARTS = 2
BF, F32 = jnp.bfloat16, jnp.float32


def norm_rows(z, gain, bias):
    wide = z.astype(F32)
    mean = jnp.mean(wide, axis=1, keepdims=True)
    centred = wide - mean
    var = jnp.mean(centred * centred, axis=1, keepdims=True)
    return centred * lax.rsqrt(var + 1e-05) * gain + bias


def sigmoid(x):
    return 0.5 * jnp.tanh(0.5 * x) + 0.5


def pick(parts, odd, high):
    return jnp.where(high, jnp.where(odd, parts[3], parts[2]), jnp.where(odd, parts[1], parts[0]))


def swap_blocks(x):
    lane = lax.broadcasted_iota(jnp.int32, x[0].shape, 1)
    odd, high = (lane // 32) % 2 == 1, lane >= 64
    skew = [pick([x[(b + d) % 4] for b in range(4)], odd, high) for d in range(4)]
    turned = [skew[0]] + [pltpu.roll(skew[d], 32 * d, 1) for d in range(1, 4)]
    return [pick([turned[(b - a) % 4] for b in range(4)], odd, high) for a in range(4)]


def tri_kernel(in_ref, out_hbm, mlb, mrb, tri, stage, sems, *, incoming):
    top = lax.broadcasted_iota(jnp.int32, (8, C), 0) < 4

    def gather(r, carry):
        whole = [in_ref[r * COLS + c].astype(F32) for c in range(COLS)]
        for v in range(6):
            x = []
            for b in range(4):
                c, h = divmod(4 * v + b, KHI)
                x.append(whole[c][h * 24:(h + 1) * 24, :])
            y = swap_blocks(x)
            tail = [z[16:24] for z in y]
            left, right = [z[0:8] for z in y], [z[8:16] for z in y]
            for a in (0, 2):
                left.append(jnp.where(top, tail[a], pltpu.roll(tail[a + 1], 4, 0)))
                right.append(jnp.where(top, pltpu.roll(tail[a], 4, 0), tail[a + 1]))
            rows, lanes = pl.ds(pl.multiple_of(r * TR, TR), TR), slice(v * C, (v + 1) * C)
            mlb[rows, lanes] = jnp.concatenate(left, axis=0).astype(BF)
            mrb[rows, lanes] = jnp.concatenate(right, axis=0).astype(BF)
        return carry

    lax.fori_loop(0, ROWS, gather, 0, unroll=4)
    for m in range(2):
        cut = slice(m * 384, (m + 1) * 384)
        if incoming:
            tri[cut, :] = lax.dot_general(
                mlb[:, cut], mrb[...], (((0,), (0,)), ((), ())), preferred_element_type=F32)
        else:
            tri[cut, :] = lax.dot_general(
                mlb[cut, :], mrb[...], (((1,), (1,)), ((), ())), preferred_element_type=F32)

    def copy_out(r):
        dests = pl.ds(r * 2 * COLS, 2 * COLS)
        return pltpu.make_async_copy(stage.at[dests], out_hbm.at[dests], sems.at[r])

    def scatter(t, carry):
        rs = (2 * t, 2 * t + 1)
        base = [pl.multiple_of(r * TR, TR) for r in rs]
        main, tail = ([], []), []
        for v in range(6):
            lanes = slice(v * C, (v + 1) * C)
            for e in range(2):
                main[e].extend(swap_blocks([tri[pl.ds(base[e] + 8 * a, 8), lanes] for a in range(4)]))
            ends = []
            for a in (32, 40):
                p, q = (tri[pl.ds(base[e] + a, 8), lanes] for e in range(2))
                ends.append(jnp.where(top, p, pltpu.roll(q, 4, 0)))
                ends.append(jnp.where(top, pltpu.roll(p, 4, 0), q))
            tail += swap_blocks(ends)
        for c in range(COLS):
            j = tail[KHI * c:KHI * c + KHI]
            last = (
                [jnp.where(top, j[0], pltpu.roll(j[1], 4, 0)), j[2]],
                [jnp.where(top, pltpu.roll(j[0], 4, 0), j[1]), pltpu.roll(j[2], 4, 0)],
            )
            for e in range(2):
                for n, piece in enumerate(main[e][KHI * c:KHI * c + KHI] + last[e]):
                    for half in range(2 if n < 4 else 1):
                        at = (2 * n + half) * C
                        stage[rs[e] * COLS + c, :, at:at + C] = piece[4 * half:4 * half + 4].astype(BF)
        copy_out(t).start()
        return carry

    lax.fori_loop(0, ROWS // 2, scatter, 0, unroll=2)

    def finish(r, carry):
        copy_out(r).wait()
        return carry

    lax.fori_loop(0, ROWS // 2, finish, 0)


def place(part):
    if part == 2:
        return TR - 16, 4, (16, 20)
    return 4 * part, 8, (4 * part, 8 + 4 * part)


def product_row(part, h):
    return 24 + 4 * h if part == 2 else 8 * h + 4 * part


def column(ref, h):
    return ref.at[:, pl.ds(pl.multiple_of(h * KLO, KLO), KLO)]


def column_in(src, dst, sems, h):
    return pltpu.make_async_copy(column(src, h), column(dst, h), sems.at[h])


def load_chunk(z, row, step, h):
    cut = pl.ds(pl.multiple_of(h * KLO, KLO), KLO)
    return jnp.concatenate([z[row + a * step, cut, :] for a in range(4)], axis=0)


def store_chunk(z, row, step, h, value):
    cut = pl.ds(pl.multiple_of(h * KLO, KLO), KLO)
    for a in range(4):
        z[row + a * step, cut, :] = value[a * KLO:(a + 1) * KLO]


def projector(chain, w, gains, biases, scr, u):
    row, col = lax.axis_index("row"), lax.axis_index("col")
    live_rows = chain[row // 2] - TR * (row % 2)
    live_cols = chain[col]
    gain, bias = gains[u, 0:1, :], biases[u, 0:1, :]
    columns = (w[u, :, 0:4 * C].astype(F32) * 0.5).T.astype(BF)
    w_t = jnp.concatenate([
        columns[(2 * side + k) * C + d:(2 * side + k) * C + d + 16]
        for side in range(2) for d in range(0, C, 16) for k in range(2)
    ], axis=0)
    lane = lax.broadcasted_iota(jnp.int32, (1, C), 1)

    def project(chunks, h, part):
        first, step, factor_rows = place(part)
        lane_row, lane_col = lane // KLO * step + first, lane % KLO + h * KLO
        for half in range(2):
            es = (2 * half, 2 * half + 1)
            normed = jnp.concatenate([norm_rows(chunks[e], gain, bias).astype(BF) for e in es], axis=0)
            mask = jnp.concatenate(
                [((lane_row + e < live_rows) & (lane_col < live_cols)).astype(F32) for e in es], axis=1)
            every = lax.dot_general(
                w_t, normed, (((1,), (1,)), ((), ())), preferred_element_type=F32)
            for side in range(2):
                for d in range(0, C, 16):
                    at = 2 * (side * C + d)
                    value, gate = every[at:at + 16], every[at + 16:at + 32]
                    edges = mask * (value * jnp.tanh(gate) + value)
                    for n, e in enumerate(es):
                        rows = pl.ds(d * SA + factor_rows[side] + e, 16, stride=SA)
                        scr[rows, :] = edges[:, n * C:(n + 1) * C]

    return project


def factors_out(stage, out, sems, h, part):
    dests = pl.ds(part * (C // PARTS), C // PARTS)
    return pltpu.make_async_copy(
        stage.at[h, dests], out.at[dests, pl.ds(pl.multiple_of(h * SA, SA), SA)], sems.at[h, part])


def send_factors(scr, stage, out, sems, h):
    def cast(s, carry):
        stage[h, s] = scr[pl.ds(pl.multiple_of(s * SA, SA), SA), :].astype(BF)
        return carry

    for part in range(PARTS):
        lax.fori_loop(part * (C // PARTS), (part + 1) * (C // PARTS), cast, 0, unroll=32)
        factors_out(stage, out, sems, h, part).start()


def each_column(step):
    def one(h, carry):
        step(h)
        return carry

    lax.fori_loop(0, KHI, one, 0, unroll=True)


def pre_kernel(chain_hbm, z_hbm, w_hbm, gain_hbm, bias_hbm, out_hbm,
               chain, z, w, gains, biases, scr, stage, in_sems, z_sems, out_sems):
    small = [pltpu.make_async_copy(a, b, in_sems.at[n]) for n, (a, b) in enumerate(
        ((chain_hbm, chain), (w_hbm, w), (gain_hbm, gains), (bias_hbm, biases)))]
    for one in small + [column_in(z_hbm, z, z_sems, h) for h in range(KHI)]:
        one.start()
    for one in small:
        one.wait()
    project = projector(chain, w, gains, biases, scr, 0)

    def step(h):
        column_in(z_hbm, z, z_sems, h).wait()
        for part in range(3):
            row, gap = place(part)[:2]
            project([load_chunk(z, row + e, gap, h) for e in range(4)], h, part)
        send_factors(scr, stage, out_hbm, out_sems, h)

    each_column(step)
    for h in range(KHI):
        for part in range(PARTS):
            factors_out(stage, out_hbm, out_sems, h, part).wait()


def post_parts(prod, z_hbm, gate_hbm, gains, biases, w_out, z, gate, wide, normed, z_sems, gate_sems, u):
    for h in range(KHI):
        column_in(z_hbm, z, z_sems, h).start()
        column_in(gate_hbm, gate, gate_sems, h).start()
    gain = jnp.broadcast_to(gains[u, 1:2, :], (C, C)).T
    bias = jnp.broadcast_to(biases[u, 1:2, :], (C, C)).T

    def widen(s, carry):
        fours = [prod[s, :, n * C:(n + 1) * C].astype(F32) for n in range(NQ // 4)]
        wide[pl.ds(pl.multiple_of(s * SP, 8), NQ), :] = jnp.concatenate(fours, axis=0)
        return carry

    lax.fori_loop(0, C, widen, 0, unroll=32)

    def normalise(h):
        for part in range(3):
            for e in range(4):
                x = wide[pl.ds(product_row(part, h) + e, C, stride=SP), :]
                mean = jnp.mean(x, axis=0, keepdims=True)
                centred = x - mean
                var = jnp.mean(centred * centred, axis=0, keepdims=True)
                normed[h, 4 * part + e] = (centred * lax.rsqrt(var + 1e-05) * gain + bias).astype(BF)

    each_column(normalise)

    def update(z_out, h):
        column_in(z_hbm, z, z_sems, h).wait()
        column_in(gate_hbm, gate, gate_sems, h).wait()
        for part in range(3):
            row, gap = place(part)[:2]
            for e in range(4):
                mixed = lax.dot_general(
                    normed[h, 4 * part + e], w_out[u], (((0,), (0,)), ((), ())), preferred_element_type=F32)
                old = load_chunk(z, row + e, gap, h).astype(F32)
                new = old + load_chunk(gate, row + e, gap, h) * mixed
                store_chunk(z_out, row + e, gap, h, new.astype(BF))

    return update


def mid_kernel(chain, prod, z_hbm, gate_hbm, w, gains, biases, w_out, z_out_hbm, out_hbm,
               z, gate, wide, normed, z_out, scr, stage, z_sems, gate_sems, zo_sems, out_sems):
    update = post_parts(
        prod, z_hbm, gate_hbm, gains, biases, w_out, z, gate, wide, normed, z_sems, gate_sems, 0)
    project = projector(chain, w, gains, biases, scr, 1)

    def renew(h):
        update(z_out, h)
        column_in(z_out, z_out_hbm, zo_sems, h).start()

    def step(h):
        for part in range(3):
            row, gap = place(part)[:2]
            project([load_chunk(z_out, row + e, gap, h) for e in range(4)], h, part)
        send_factors(scr, stage, out_hbm, out_sems, h)

    each_column(renew)
    each_column(step)
    for h in range(KHI):
        column_in(z_out, z_out_hbm, zo_sems, h).wait()
        for part in range(PARTS):
            factors_out(stage, out_hbm, out_sems, h, part).wait()


def post_kernel(prod, z_hbm, gate_hbm, gains, biases, w_out, z_out_hbm,
                z, gate, wide, normed, z_out, z_sems, gate_sems, zo_sems):
    update = post_parts(
        prod, z_hbm, gate_hbm, gains, biases, w_out, z, gate, wide, normed, z_sems, gate_sems, 1)

    def step(h):
        update(z_out, h)
        column_in(z_out, z_out_hbm, zo_sems, h).start()

    each_column(step)
    for h in range(KHI):
        column_in(z_out, z_out_hbm, zo_sems, h).wait()


HBM = pl.BlockSpec(memory_space=pltpu.HBM)
VMEM = pl.BlockSpec(memory_space=pltpu.VMEM)
SMEM = pl.BlockSpec(memory_space=pltpu.SMEM)
FACTORS, PRODUCTS, STATE = ((C, 2 * NQ, C), BF), ((C, 4, NQ // 4 * C), BF), ((TR, TC, C), BF)


def call(kernel, name, outs, scratch, sems, limit, in_specs):
    shapes = [pltpu.HBM(*o) for o in outs]
    run = pl.pallas_call(
        kernel,
        out_shape=shapes if len(shapes) > 1 else shapes[0],
        in_specs=in_specs,
        out_specs=[HBM] * len(shapes) if len(shapes) > 1 else HBM,
        scratch_shapes=list(scratch) + [pltpu.SemaphoreType.DMA(n if isinstance(n, tuple) else (n,)) for n in sems],
        compiler_params=pltpu.CompilerParams(vmem_limit_bytes=limit << 20),
        name=name,
    )

    def placed(*args):
        return run(*(
            pltpu.with_memory_space_constraint(a, s.memory_space)
            if s is HBM or (s is VMEM and a.size > N * N) else a
            for a, s in zip(args, in_specs)
        ))

    return placed


def kernels():
    V = pltpu.VMEM
    send = [V((C * SA, C), F32), V((KHI, C, SA, C), BF)]
    pre = call(
        pre_kernel, "pre", [FACTORS],
        [pltpu.SMEM((8,), jnp.int32), V(*STATE), V((2, C, 5 * C), BF), V((2, 2, C), F32), V((2, 2, C), F32)] + send,
        [4, KHI, (KHI, PARTS)], 20, [HBM] * 5)
    tri = [
        call(
            functools.partial(tri_kernel, incoming=u == 1), "tri", [PRODUCTS],
            [V((N, N), BF), V((N, N), BF), V((N, N), F32), V(*PRODUCTS)], [ROWS // 2], 20, [VMEM])
        for u in range(2)
    ]
    take = [V(*STATE), V(STATE[0], F32), V((C * SP, C), F32), V((KHI, 12, C, C), BF), V(*STATE)]
    mid = call(
        mid_kernel, "mid", [STATE, FACTORS], take + send, [KHI, KHI, KHI, (KHI, PARTS)], 26,
        [SMEM, VMEM] + [HBM] * 2 + [VMEM] * 4)
    post = call(
        post_kernel, "post", [STATE], take, [KHI, KHI, KHI], 16, [VMEM] + [HBM] * 2 + [VMEM] * 3)
    return pre, tri, mid, post


def output_gate(state, w_in, gains, biases, u):
    normed = norm_rows(state.reshape(-1, C), gains[u, 0], biases[u, 0]).astype(BF)
    gate = jax.nn.sigmoid(jnp.dot(normed, w_in[u, :, 4 * C:], preferred_element_type=F32))
    return gate.reshape(state.shape)


def body(pair, chain_lengths, gains, biases, w_in, w_out):
    def exchange(blocks):
        return lax.all_to_all(blocks, ("row", "col"), 0, 0, tiled=True)

    pre, tri, mid, post = kernels()
    factors = exchange(pre(chain_lengths, pair, w_in, gains, biases))
    gate = output_gate(pair, w_in, gains, biases, 0)
    products = exchange(tri[0](factors))
    state, factors = mid(chain_lengths, products, pair, gate, w_in, gains, biases, w_out)
    factors = exchange(factors)
    gate = output_gate(state, w_in, gains, biases, 1)
    products = exchange(tri[1](factors))
    return post(products, state, gate, gains, biases, w_out)


def solution(mesh):
    placed = (P("row", "col", None), P(), P(), P(), P(), P())
    return jax.shard_map(
        body, mesh=mesh, in_specs=placed, out_specs=P("row", "col", None), check_vma=False
    )
```
